32 devices in a mesh: row: 4 (over y, x), col: 8 (over z, core).
Axes of the slice: x: 2, y: 2, z: 4, core: 2. Of those that a mesh axis runs over, the one named last changes fastest.
Arguments:
- amplitudes: bfloat16 [800, 800, 768], P('row', 'col'), may hold values from -6 to 6
- integrals: bfloat16 [800, 800, 256], P('row', 'col'), may hold values from -0.375 to 0.375
- window_index: int32 [256], replicated, may hold values from 0 to 639999, as said below
Outputs:
- residual: bfloat16 [800, 800, 768], P('row', 'col')
- pair_energy: float32 [768], replicated
The draws below stay inside these ranges and needn't reach their ends.
Inputs may be any that keep to these rules, and one draw needn't show every extreme that they name: `window_index`: the window pairs are distinct; pair k lies in the block of a rows and b columns owned by device number k // 8 in row-major order of the (a, b) device grid, 8 pairs for each block.
All inputs are finite; a program needn't handle non-finite values.
Results may differ from the reference program's by a relative error of at most 0.001.
Values may be sent and summed in bfloat16 or wider, within the bound.
A program may use at most 256 MiB of HBM per device.

```python
import jax
import jax.numpy as jnp
from jax import lax

VIRT = 800
PAIRS = 768
KD = 8
WINDOW = 256
N_ROW = 4
N_COL = 8


def draw_window_index(key, part):
    block_rows = VIRT // N_ROW
    block_cols = VIRT // N_COL
    device_keys = jax.random.split(jax.random.fold_in(key, 17), N_ROW * N_COL)

    def choose_cells(one_key):
        return jax.random.permutation(one_key, block_rows * block_cols)[:KD].astype(jnp.int32)
    picked = jax.vmap(choose_cells)(device_keys)
    device_ids = jnp.arange(N_ROW * N_COL, dtype=jnp.int32)
    row_ids = device_ids // N_COL
    col_ids = device_ids % N_COL
    a_index = row_ids[:, None] * block_rows + picked // block_cols
    b_index = col_ids[:, None] * block_cols + picked % block_cols
    return (a_index * VIRT + b_index).reshape(-1).astype(jnp.int32)


def level_of(stream_key, extent, pieces, least, high):
    level = 1.0
    for dim, blocks in pieces:
        draws = jax.random.uniform(jax.random.fold_in(jax.random.fold_in(stream_key, 6), dim), (blocks,), jnp.float32, least / len(pieces), high / len(pieces))
        level = level * jnp.repeat(jnp.exp(draws), extent[dim] // blocks).reshape((-1,) + (1,) * (len(extent) - 1 - dim))
    return level


def gaussian(key, shape, width, most, pieces=(), kind=jnp.bfloat16):
    entries = jax.random.normal(key, shape, jnp.float32) * width
    if len(pieces) > 0:
        entries = level_of(key, shape, pieces, -0.22, 0.18) * entries
    return jnp.clip(entries, min=-most, max=most).astype(kind)


def setup_inputs(seed: int = 0) -> dict:
    seeds = jax.random.split(jax.random.key(seed), 4)
    amplitudes = gaussian(seeds[0], (VIRT, VIRT, PAIRS), 1.0, 6.0, ((0, 4), (1, 8)))
    integrals = gaussian(seeds[1], (VIRT, VIRT, WINDOW), WINDOW ** -0.5, 0.375, ((0, 4), (1, 8)))
    window_index = draw_window_index(jax.random.fold_in(seeds[3], 71), 0)
    return dict(amplitudes=amplitudes, integrals=integrals, window_index=window_index)


def reference(amplitudes, integrals, window_index):
    flattened = amplitudes.reshape(VIRT * VIRT, PAIRS)
    columns = jnp.take(flattened, window_index, axis=0)
    block_rows = VIRT // N_ROW

    def one_block(block_index):
        start = (block_index * block_rows).astype(jnp.int32)
        part_ints = lax.dynamic_slice_in_dim(integrals, start, block_rows, 0)
        part_amps = lax.dynamic_slice_in_dim(amplitudes, start, block_rows, 0)
        full = jnp.dot(part_ints.reshape(block_rows * VIRT, WINDOW), columns, preferred_element_type=jnp.float32)
        energy = jnp.sum(part_amps.reshape(block_rows * VIRT, PAIRS).astype(jnp.float32) * full, axis=0)
        return full.astype(jnp.bfloat16), energy

    blocks, energies = lax.map(one_block, jnp.arange(N_ROW, dtype=jnp.int32))
    residual = blocks.reshape(VIRT, VIRT, PAIRS)
    pair_energy = jnp.sum(energies, axis=0) / VIRT
    return residual, pair_energy
```

```python
import functools

import jax
import jax.numpy as jnp
from jax import lax
from jax.experimental import pallas as pl
from jax.experimental.pallas import tpu as pltpu
from jax.sharding import PartitionSpec as P

MESH = pl.DeviceIdType.MESH
ROWS = 2000
OUT_ROWS = 1000
MIB = 1024 * 1024


def largest_divisor(extent, most, multiple):
    fits = [d for d in range(multiple, min(extent, most) + 1, multiple) if extent % d == 0]
    return max(fits) if fits else extent


def gather_kernel(
    nrows, ncols, rows, own_ref, ints_ref, amps_ref, out_ref, energy_ref,
    held, product, partial, values, load_sems, send_sems, recv_sems, esend_sems, erecv_sems,
):
    count = nrows * ncols
    cells = ints_ref.shape[0]
    chunks = cells // rows
    me = lax.axis_index("row") * ncols + lax.axis_index("col")

    def place(step):
        other = lax.rem(me + step, count)
        return (other // ncols, lax.rem(other, ncols))

    def load(i):
        span = pl.ds(i * rows, rows)
        return pltpu.make_async_copy(amps_ref.at[span], held.at[span], load_sems.at[i])

    for i in range(chunks):
        load(i).start()

    barrier = pltpu.get_barrier_semaphore()

    def greet(step, carry):
        pl.semaphore_signal(barrier, inc=1, device_id=place(step), device_id_type=MESH)
        return carry

    lax.fori_loop(1, count, greet, 0)

    def block(i):
        span = pl.ds(pl.multiple_of(i * rows, rows), rows)
        return lax.dot_general(
            ints_ref[span], held[span], (((0,), (0,)), ((), ())), preferred_element_type=jnp.float32
        )

    load(0).wait()
    product[...] = block(0)

    pl.semaphore_wait(barrier, count - 1)

    def copy(step, slot):
        return pltpu.make_async_remote_copy(
            src_ref=own_ref,
            dst_ref=out_ref.at[slot],
            send_sem=send_sems.at[step],
            recv_sem=recv_sems.at[step],
            device_id=place(step),
            device_id_type=MESH,
        )

    def send(step, carry):
        copy(step, me).start()
        return carry

    lax.fori_loop(1, count, send, 0)
    out_ref[me] = own_ref[...]

    def accumulate(i, carry):
        load(i).wait()
        product[...] += block(i)
        return carry

    lax.fori_loop(1, chunks, accumulate, 0)

    def finish(step, carry):
        source = lax.rem(me + count - step, count)
        copy(step, source).wait_recv()
        copy(step, me).wait_send()
        return carry

    lax.fori_loop(1, count, finish, 0)

    per_device = own_ref.shape[0]
    total = jnp.zeros(own_ref.shape, jnp.float32)
    for d in range(count):
        total = total + out_ref[d].astype(jnp.float32) * product[d * per_device : (d + 1) * per_device]
    partial[...] = jnp.sum(total, axis=0, keepdims=True)

    def ecopy(step, slot):
        return pltpu.make_async_remote_copy(
            src_ref=partial,
            dst_ref=values.at[slot],
            send_sem=esend_sems.at[step],
            recv_sem=erecv_sems.at[step],
            device_id=place(step),
            device_id_type=MESH,
        )

    def esend(step, carry):
        ecopy(step, me).start()
        return carry

    lax.fori_loop(1, count, esend, 0)
    values[me] = partial[...]

    def efinish(step, carry):
        source = lax.rem(me + count - step, count)
        ecopy(step, source).wait_recv()
        ecopy(step, me).wait_send()
        return carry

    lax.fori_loop(1, count, efinish, 0)
    energy_ref[...] = jnp.sum(values[...], axis=0)


def gather(owned, integrals, amplitudes, nrows, ncols):
    count = nrows * ncols
    cells, pairs = amplitudes.shape
    window = integrals.shape[1]
    rows = largest_divisor(cells, ROWS, 8)
    size = amplitudes.dtype.itemsize
    limit = cells * pairs * size + 4 * window * pairs * 4 + 4 * MIB
    vmem = pl.BlockSpec(memory_space=pltpu.VMEM)
    dma = pltpu.SemaphoreType.DMA
    return pl.pallas_call(
        functools.partial(gather_kernel, nrows, ncols, rows),
        out_shape=(
            jax.ShapeDtypeStruct((count,) + owned.shape, owned.dtype),
            jax.ShapeDtypeStruct((1, pairs), jnp.float32),
        ),
        in_specs=[vmem, vmem, pl.BlockSpec(memory_space=pl.ANY)],
        out_specs=(vmem, vmem),
        scratch_shapes=[
            pltpu.VMEM((cells, pairs), amplitudes.dtype),
            pltpu.VMEM((window, pairs), jnp.float32),
            pltpu.VMEM((1, pairs), jnp.float32),
            pltpu.VMEM((count, 1, pairs), jnp.float32),
            dma((cells // rows,)),
            dma((count,)),
            dma((count,)),
            dma((count,)),
            dma((count,)),
        ],
        compiler_params=pltpu.CompilerParams(
            collective_id=0, has_side_effects=True, vmem_limit_bytes=limit
        ),
    )(owned, integrals, amplitudes)


def residual_kernel(ints_ref, cols_ref, out_ref):
    rows = out_ref.shape[0]
    start = pl.multiple_of(pl.program_id(0) * rows, 8)
    full = jnp.dot(ints_ref[pl.ds(start, rows)], cols_ref[...], preferred_element_type=jnp.float32)
    out_ref[...] = full.astype(out_ref.dtype)


def multiply(integrals, columns):
    cells, window = integrals.shape
    pairs = columns.shape[1]
    rows = largest_divisor(cells, OUT_ROWS, 8)
    vmem = pl.BlockSpec(memory_space=pltpu.VMEM)
    return pl.pallas_call(
        residual_kernel,
        grid=(cells // rows,),
        out_shape=jax.ShapeDtypeStruct((cells, pairs), jnp.bfloat16),
        in_specs=[vmem, vmem],
        out_specs=pl.BlockSpec((rows, pairs), lambda i: (i, 0)),
        compiler_params=pltpu.CompilerParams(
            dimension_semantics=("arbitrary",), vmem_limit_bytes=24 * MIB
        ),
    )(integrals, columns)


def shards(amplitudes, integrals, window_index):
    block_rows, block_cols, pairs = amplitudes.shape
    window = integrals.shape[2]
    ncols = lax.axis_size("col")
    nrows = lax.axis_size("row")
    per_device = window // (nrows * ncols)
    row_rank = lax.axis_index("row")
    col_rank = lax.axis_index("col")
    linear_rank = row_rank * ncols + col_rank
    owned_index = lax.dynamic_slice_in_dim(window_index, linear_rank * per_device, per_device)
    virtuals = block_rows * nrows
    row_offset = owned_index // virtuals - row_rank * block_rows
    col_offset = owned_index % virtuals - col_rank * block_cols
    owned = amplitudes[row_offset, col_offset]
    cells = block_rows * block_cols
    flat_ints = integrals.transpose(1, 0, 2).reshape(cells, window)
    columns, energy = gather(
        owned, flat_ints, amplitudes.transpose(1, 0, 2).reshape(cells, pairs), nrows, ncols
    )
    residual = multiply(flat_ints, columns.reshape(window, pairs))
    residual = residual.reshape(block_cols, block_rows, pairs).transpose(1, 0, 2)
    return (residual, energy[0] / virtuals)


def solution(mesh):
    return jax.shard_map(
        shards,
        mesh=mesh,
        in_specs=(P("row", "col", None), P("row", "col", None), P()),
        out_specs=(P("row", "col", None), P()),
        check_vma=False,
    )
```
